1024 devices in a mesh: expert: 16 (over x, y_hi, core), fsdp: 64 (over y_lo, z).
Axes of the slice: x: 4, y: 8 (y_hi: 2, y_lo: 4; y = y_hi * 4 + y_lo), z: 16, core: 2. Of those that a mesh axis runs over, the one named last changes fastest.
Arguments:
- momentum: float32 [16, 7168, 1024], P(None, ('fsdp', 'expert')), may hold values from -6 to 6
- spectral_sq: float32 [16], P('expert'), may hold values from 10752 to 35840
Outputs:
- update: bfloat16 [16, 7168, 1024], P(None, ('fsdp', 'expert'))
The draws below stay inside these ranges and needn't reach their ends.
All inputs are finite; a program needn't handle non-finite values.
Results may differ from the reference program's by a relative error of at most 0.0064.
Values may be sent and summed in bfloat16 or wider, within the bound.
A program may use at most 32 MiB of HBM per device.

```python
import math
import jax
import jax.numpy as jnp
from jax import lax

C = 7168
R = 1024
EXPERTS = 16


def draw_momentum(key, part):
    first_key = jax.random.fold_in(key, 11)
    values = jax.random.normal(first_key, (EXPERTS, C, R), jnp.float32)
    return jnp.clip(values, -6.0, 6.0)


def block_levels(key, dims, cuts, smallest, top_value):
    loudness = 1.0
    for position, shards_of in cuts:
        steps = jax.random.uniform(jax.random.fold_in(jax.random.fold_in(key, 6), position), (shards_of,), jnp.float32, smallest / len(cuts), top_value / len(cuts))
        loudness = loudness * jnp.repeat(jnp.exp(steps), dims[position] // shards_of).reshape((-1,) + (1,) * (len(dims) - 1 - position))
    return loudness


def setup_inputs(seed: int = 0) -> dict:
    arg_keys = jax.random.split(jax.random.key(seed), 3)
    momentum = draw_momentum(jax.random.fold_in(arg_keys[2], 71), 0)
    spectral_sq = jnp.clip(jnp.exp(math.log(35840.0) - 1.2039728 * jax.random.uniform(arg_keys[1], (EXPERTS,), jnp.float32) ** block_levels(arg_keys[1], (EXPERTS,), ((0, 16),), -0.2, 0.2)), 10752.0, 35840.0)
    return dict(momentum=momentum, spectral_sq=spectral_sq)


coef_a = 3.4445
coef_b = -4.775
coef_c = 2.0315

def one_matrix(pieces):
    matrix, square = pieces
    scaled = (matrix / jnp.sqrt(square)).astype(jnp.bfloat16)
    gram_sum = jnp.dot(scaled.T, scaled, preferred_element_type=jnp.float32)
    rounded = gram_sum.astype(jnp.bfloat16)
    product = jnp.dot(rounded, rounded, preferred_element_type=jnp.float32)
    polynomial = (coef_b * rounded.astype(jnp.float32) + coef_c * product).astype(jnp.bfloat16)
    update = coef_a * scaled.astype(jnp.float32) + jnp.dot(scaled, polynomial, preferred_element_type=jnp.float32)
    return (update * jnp.sqrt(jnp.float32(C))).astype(jnp.bfloat16)

def reference(momentum, spectral_sq):
    return lax.map(one_matrix, (momentum, spectral_sq))
```

```python
import jax
import jax.numpy as jnp
from jax import lax
from jax.experimental import pallas as pl
from jax.experimental.pallas import tpu as pltpu
from jax.sharding import Mesh
from jax.sharding import PartitionSpec as P

C = 7168
coef_a = 3.4445
coef_b = -4.775
coef_c = 2.0315

AXES = ("x", "yh", "core", "yl", "z")
MESH = pl.DeviceIdType.MESH
LANES = 128
f32 = jnp.float32
bf16 = jnp.bfloat16


def kernel(
    sizes, m_hbm, s_ref, o_ref,
    m_ref, msend, xin, xe, own, psend, precv, acc, qsend, qrecv,
    stored, gram, poly, zrow, osend, sq,
    m_sem, zs, zr, cs, cr, xs, xr, ys, yr, gys, gyr, gxs, gxr, gcs, gcr, os, orv,
    ss, sr,
):
    nx, ny, nz, nyl = sizes
    nb = 2 * nx
    nd = nb // 2 + 1
    x, yh, c, yl, z = [lax.axis_index(a) for a in AXES]
    y = yh * nyl + yl
    expert = (x * 2 + yh) * 2 + c
    part = ny and LANES // ny

    def to_z(d):
        return {"z": lax.rem(z + d, nz)}

    def to_x(d):
        return {"x": lax.rem(x + d, nx)}

    def to_y(d):
        t = lax.rem(y + d, ny)
        return {"yh": t // nyl, "yl": lax.rem(t, nyl)}

    to_core = {"core": 1 - c}

    def far_first(k, n):
        h = (k + 1) // 2
        return n // 2 + h * (1 - 2 * lax.rem(k, 2))

    load = pltpu.make_async_copy(m_hbm, m_ref, m_sem)
    load.start()

    barrier = pltpu.get_barrier_semaphore()

    def greet(k, carry):
        pl.semaphore_signal(barrier, inc=1, device_id=to_z(far_first(k, nz)), device_id_type=MESH)
        return carry

    lax.fori_loop(0, nz - 1, greet, 0)
    for d in range(1, ny):
        pl.semaphore_signal(barrier, inc=1, device_id=to_y(d), device_id_type=MESH)
    for d in range(1, nx):
        pl.semaphore_signal(barrier, inc=1, device_id=to_x(d), device_id_type=MESH)
    pl.semaphore_signal(barrier, inc=1, device_id=to_core, device_id_type=MESH)

    sq[0] = jnp.full(sq.shape[1:], jnp.where(expert == z, s_ref[0], 0.0), f32)
    load.wait()

    def padded(e):
        rows = m_ref[e]
        return jnp.concatenate([rows, jnp.zeros((1, rows.shape[1]), f32)], 0).astype(bf16)

    def cast(e, carry):
        msend[e] = padded(e)
        return carry

    lax.fori_loop(0, nz, cast, 0)
    xin[0, 0] = padded(z)

    pl.semaphore_wait(barrier, (nz - 1) + (ny - 1) + (nx - 1) + 1)

    def remote(src, dst, send_sem, recv_sem, where):
        return pltpu.make_async_remote_copy(
            src_ref=src, dst_ref=dst, send_sem=send_sem, recv_sem=recv_sem,
            device_id=where, device_id_type=MESH,
        )

    def z_copy(d):
        return remote(
            msend.at[lax.rem(z + d, nz)], xin.at[0, d], zs.at[d], zr.at[d], to_z(d)
        )

    def swap_copy(d):
        return remote(xin.at[0, d], xin.at[1, d], cs.at[d], cr.at[d], to_core)

    def z_start(k, carry):
        z_copy(far_first(k, nz)).start()
        return carry

    lax.fori_loop(0, nz - 1, z_start, 0)
    swap_copy(0).start()
    sq_core = remote(sq.at[0], sq.at[1], ss.at[0], sr.at[0], to_core)
    sq_core.start()

    def z_take(k, carry):
        d = nz - 1 - k
        d = lax.rem(far_first(nz - 2 - k, nz), nz)
        z_copy(d).wait_recv()
        swap_copy(d).start()
        return carry

    lax.fori_loop(0, nz - 1, z_take, 0)

    width = nb * LANES
    extra = (nd - 1) * LANES
    half = nz * 8

    def spread(side, k):
        pair = jnp.concatenate(
            [xin[side, 2 * k].astype(f32), xin[side, 2 * k + 1].astype(f32)], 0
        ).astype(bf16)
        rows = pl.ds(pl.multiple_of(side * half + k * 16, 16), 16)
        xe[rows, :width] = pair
        xe[rows, width:] = pair[:, :extra]

    def spread_own(k, carry):
        spread(0, k)
        return carry

    def spread_other(k, carry):
        spread(1, k)
        return carry

    lax.fori_loop(0, nz // 2, spread_own, 0)

    def swap_take(d, carry):
        swap_copy(d).wait_recv()
        return carry

    lax.fori_loop(0, nz, swap_take, 0)
    lax.fori_loop(0, nz // 2, spread_other, 0)

    sq_core.wait_recv()
    sq[2] = sq[0] + sq[1]

    def x_copy(d):
        return remote(psend.at[d], precv.at[d], xs.at[d], xr.at[d], to_x(d))

    def sq_x(d):
        return remote(sq.at[2], sq.at[2 + d], ss.at[d], sr.at[d], to_x(d))

    def partial_gram(d):
        start = pl.multiple_of((2 * lax.rem(x + d, nx) + c) * LANES, LANES)
        return lax.dot_general(
            xe[:, pl.ds(start, LANES)], xe[:, pl.ds(start, nd * LANES)],
            (((0,), (0,)), ((), ())), preferred_element_type=f32,
        )

    order_x = sorted(range(1, nx), key=lambda d: -min(d, nx - d))
    for d in order_x:
        psend[d] = partial_gram(d).astype(bf16)
        x_copy(d).start()
    for d in order_x:
        sq_x(d).start()
    total = partial_gram(0)
    for d in reversed(order_x):
        x_copy(d).wait_recv()
        total = total + precv[d].astype(f32)
    total = total.reshape(acc.shape)
    acc[...] = total
    qsend[...] = total.astype(bf16)

    def y_copy(d):
        return remote(
            qsend.at[lax.rem(y + d, ny)], qrecv.at[d], ys.at[d], yr.at[d], to_y(d)
        )

    order_y = sorted(range(1, ny), key=lambda d: -min(d, ny - d))
    for d in order_y:
        y_copy(d).start()
    s_sum = sq[2]
    for d in order_x:
        sq_x(d).wait_recv()
        s_sum = s_sum + sq[2 + d]
    sq[nx + 2] = s_sum
    sq_y = remote(sq.at[nx + 2], sq.at[nx + 3], ss.at[nx], sr.at[nx], to_y(ny // 2))
    sq_y.start()

    total = acc[y]
    for d in reversed(order_y):
        y_copy(d).wait_recv()
        total = total + qrecv[d].astype(f32)
    sq_y.wait_recv()
    square = sq[nx + 2] + sq[nx + 3]
    inverse = jnp.concatenate([1.0 / square] * nd, 1)
    inverse = jnp.concatenate([inverse] * (part // 8), 0)
    mine = 2 * x + c
    stored[mine, y] = (total * inverse).astype(bf16)

    def gy_copy(d, slot):
        return remote(stored.at[mine, slot], stored.at[mine, slot], gys.at[d], gyr.at[d], to_y(d))

    for d in order_y:
        gy_copy(d, y).start()
    for d in reversed(order_y):
        gy_copy(d, lax.rem(y + ny - d, ny)).wait_recv()

    def block_of(d):
        return 2 * lax.rem(x + nx - d, nx) + c

    def gx_copy(d, slot):
        return remote(stored.at[slot], stored.at[slot], gxs.at[d], gxr.at[d], to_x(d))

    def gc_copy(d, slot):
        return remote(stored.at[slot], stored.at[slot], gcs.at[d], gcr.at[d], to_core)

    for d in order_x:
        gx_copy(d, mine).start()
    gc_copy(0, mine).start()

    def assemble(i):
        rows = pl.ds(pl.multiple_of(i * LANES, LANES), LANES)
        block = stored[i].reshape(LANES, nd * LANES)
        for d in range(nd):
            t = pl.multiple_of(lax.rem(i + d, nb) * LANES, LANES)
            piece = block[:, d * LANES : (d + 1) * LANES]
            gram[rows, pl.ds(t, LANES)] = piece
            if 0 < d < nd - 1:
                gram[pl.ds(t, LANES), rows] = piece.T

    assemble(mine)

    def other(d):
        return 2 * lax.rem(x + nx - d, nx) + 1 - c

    gc_copy(0, other(0)).wait_recv()
    assemble(other(0))
    for d in reversed(order_x):
        gx_copy(d, block_of(d)).wait_recv()
        gc_copy(d, block_of(d)).start()
        assemble(block_of(d))
    for d in reversed(order_x):
        gc_copy(d, other(d)).wait_recv()
        assemble(other(d))

    tile = 256

    def poly_rows(r, carry):
        rows = pl.ds(pl.multiple_of(r * tile, tile), tile)
        g = gram[rows, :]
        square_rows = jnp.dot(g, gram[...], preferred_element_type=f32)
        poly[rows, :] = (coef_b * g.astype(f32) + coef_c * square_rows).astype(bf16)
        return carry

    lax.fori_loop(0, width // tile, poly_rows, 0)

    mat = xe[:half, :width]
    zrow[...] = coef_a * mat.astype(f32) + jnp.dot(mat, poly[...], preferred_element_type=f32)
    scale = jnp.concatenate([jnp.sqrt(f32(C)) / jnp.sqrt(square)] * nb, 1)

    def out_value(d):
        rows = pl.ds(pl.multiple_of(d * 8, 8), 8)
        return (zrow[rows, :] * scale).astype(bf16)

    def o_copy(d):
        return remote(
            osend.at[d], o_ref.at[z], os.at[d], orv.at[d], {"z": lax.rem(z + nz - d, nz)}
        )

    def o_start(k, carry):
        d = far_first(k, nz)
        osend[d] = out_value(d)
        o_copy(d).start()
        return carry

    lax.fori_loop(0, nz - 1, o_start, 0)
    osend[0] = out_value(0)
    keep = pltpu.make_async_copy(osend.at[0], o_ref.at[z], m_sem)
    keep.start()

    def z_sent(d, carry):
        z_copy(d).wait_send()
        swap_copy(d).wait_send()
        return carry

    lax.fori_loop(1, nz, z_sent, 0)
    swap_copy(0).wait_send()
    sq_core.wait_send()
    sq_y.wait_send()
    for d in order_x:
        x_copy(d).wait_send()
        sq_x(d).wait_send()
        gx_copy(d, mine).wait_send()
        gc_copy(d, block_of(d)).wait_send()
    gc_copy(0, mine).wait_send()
    for d in order_y:
        y_copy(d).wait_send()
        gy_copy(d, y).wait_send()

    def o_take(k, carry):
        d = far_first(nz - 2 - k, nz)
        source = lax.rem(z + d, nz)
        remote(
            osend.at[d], o_ref.at[source], os.at[d], orv.at[d], {"z": lax.rem(z + nz - d, nz)}
        ).wait()
        return carry

    lax.fori_loop(0, nz - 1, o_take, 0)
    keep.wait()


def on_device(sizes, momentum, spectral_sq):
    nx, ny, nz, _ = sizes
    nb = 2 * nx
    nd = nb // 2 + 1
    rows, width = momentum.shape[1:]
    assert momentum.shape[0] == nz and width == nb * LANES and rows == 7
    part = LANES // ny
    sem = pltpu.SemaphoreType.DMA
    vmem = pltpu.VMEM
    out = pl.pallas_call(
        lambda *refs: kernel(sizes, *refs),
        out_shape=jax.ShapeDtypeStruct((nz, 8, width), bf16),
        in_specs=[
            pl.BlockSpec(memory_space=pl.ANY),
            pl.BlockSpec(memory_space=pltpu.SMEM),
        ],
        out_specs=pl.BlockSpec(memory_space=pl.ANY),
        scratch_shapes=[
            vmem(momentum.shape, f32),
            vmem((nz, 8, width), bf16),
            vmem((2, nz, 8, width), bf16),
            vmem((2 * nz * 8, width + (nd - 1) * LANES), bf16),
            vmem((8, LANES), f32),
            vmem((nx, LANES, nd * LANES), bf16),
            vmem((nx, LANES, nd * LANES), bf16),
            vmem((ny, part, nd * LANES), f32),
            vmem((ny, part, nd * LANES), bf16),
            vmem((ny, part, nd * LANES), bf16),
            vmem((nb, ny, part, nd * LANES), bf16),
            vmem((width, width), bf16),
            vmem((width, width), bf16),
            vmem((nz * 8, width), f32),
            vmem((nz, 8, width), bf16),
            vmem((nx + 4, 8, LANES), f32),
            sem(()),
            sem((nz,)), sem((nz,)), sem((nz,)), sem((nz,)),
            sem((nx,)), sem((nx,)), sem((ny,)), sem((ny,)),
            sem((ny,)), sem((ny,)), sem((nx,)), sem((nx,)),
            sem((nx,)), sem((nx,)), sem((nz,)), sem((nz,)),
            sem((nx + 1,)), sem((nx + 1,)),
        ],
        compiler_params=pltpu.CompilerParams(
            collective_id=0, has_side_effects=True, vmem_limit_bytes=48 << 20
        ),
        name="muon_step",
    )(momentum, spectral_sq)
    return out[:, :rows]


def solution(mesh):
    ne, nf = mesh.shape["expert"], mesh.shape["fsdp"]
    nx, nyl = ne // 4, 4
    nz = nf // nyl
    sizes = (nx, 2 * nyl, nz, nyl)
    finer = Mesh(mesh.devices.reshape(nx, 2, 2, nyl, nz), AXES)
    rows = P(None, ("yl", "z", "x", "yh", "core"), None)
    return jax.shard_map(
        lambda m, s: on_device(sizes, m, s),
        mesh=finer,
        in_specs=(rows, P(("x", "yh", "core"))),
        out_specs=rows,
        check_vma=False,
    )
```

```python
import jax
import jax.numpy as jnp
from jax import lax
from jax.experimental import pallas as pl
from jax.experimental.pallas import tpu as pltpu
from jax.sharding import Mesh
from jax.sharding import PartitionSpec as P

C = 7168
coef_a = 3.4445
coef_b = -4.775
coef_c = 2.0315

AXES = ("x", "yh", "core", "yl", "z")
MESH = pl.DeviceIdType.MESH
LANES = 128
ROWS = 7
f32 = jnp.float32
bf16 = jnp.bfloat16

CHUNKS = (1, 2, 3, 4, 0)
STEPS = (
    "X0 X1 X2 Y0 X3 Y1 X4 Y2 A0 Y3 A1 Y4 A2 B0 A3 B1 A4 B2 B3 B4".split()
)
OUT_CUTS = (0, 384, 896)


def row_of(shape):
    return lax.broadcasted_iota(jnp.int32, shape, 0)


def spread_rows(last):
    return jnp.concatenate(
        [jnp.broadcast_to(last[j : j + 1], (8, LANES)) for j in range(ROWS)], 1
    )


def last_block(packed):
    out = jnp.zeros((8, LANES), f32)
    row = row_of(out.shape)
    for j in range(ROWS):
        piece = packed[ROWS : ROWS + 1, j * LANES : (j + 1) * LANES]
        out = jnp.where(row == j, jnp.broadcast_to(piece, out.shape), out)
    return out


def kernel(
    sizes, m_hbm, s_ref, o_ref,
    m_ref, msend, xin, xe, xb, psend, precv, own, acc, qsend, qrecv,
    stored, gram, poly, zrow, tail, osend, orecv, sq,
    m_sem, zs, zr, cs, cr, xs, xr, ys, yr, gys, gyr, gxs, gxr, gcs, gcr, os, orv,
    ss, sr,
):
    nx, ny, nz, nyl = sizes
    nb = 2 * nx
    nd = nb // 2 + 1
    x, yh, c, yl, z = [lax.axis_index(a) for a in AXES]
    y = yh * nyl + yl
    expert = (x * 2 + yh) * 2 + c
    part = LANES // ny
    width = nb * LANES
    short = ROWS * LANES
    half = nz * 8
    order_x = sorted(range(1, nx), key=lambda d: -min(d, nx - d))
    pending = []

    def to_z(d):
        return {"z": lax.rem(z + d, nz)}

    def to_x(d):
        return {"x": lax.rem(x + d, nx)}

    def to_y(d):
        t = lax.rem(y + d, ny)
        return {"yh": t // nyl, "yl": lax.rem(t, nyl)}

    to_core = {"core": 1 - c}

    def mixed(k, n):
        g, r = jnp.maximum(k - 1, 0) // 4, lax.rem(jnp.maximum(k - 1, 0), 4)
        near = 1 + g + lax.rem(r, 2) * (n - 2 - 2 * g)
        far = n // 2 - 1 - g + lax.rem(r, 2) * (2 + 2 * g)
        return jnp.where(k == 0, n // 2, jnp.where(r < 2, near, far))

    def mixed_late(k, n):
        return mixed(lax.rem(k + 1, n - 1), n)

    def each(n, body):
        def step(k, carry):
            body(k)
            return carry

        lax.fori_loop(0, n, step, 0)

    def remote(src, dst, send_sem, recv_sem, where):
        return pltpu.make_async_remote_copy(
            src_ref=src, dst_ref=dst, send_sem=send_sem, recv_sem=recv_sem,
            device_id=where, device_id_type=MESH,
        )

    load = pltpu.make_async_copy(m_hbm, m_ref, m_sem)
    load.start()

    barrier = pltpu.get_barrier_semaphore()

    def greet(where):
        pl.semaphore_signal(barrier, inc=1, device_id=where, device_id_type=MESH)

    each(nz - 1, lambda k: greet(to_z(mixed(k, nz))))
    each(ny - 1, lambda k: greet(to_y(mixed(k, ny))))
    for d in order_x:
        greet(to_x(d))
    greet(to_core)

    sq[0] = jnp.full(sq.shape[1:], jnp.where(expert == z, s_ref[0], 0.0), f32)

    def packed(rows):
        end = jnp.concatenate([rows[j : j + 1, short:] for j in range(ROWS)], 1)
        return jnp.concatenate([rows[:, :short], end], 0).astype(bf16)

    group = min(nz, 8)

    def cast(g):
        first = pl.multiple_of(g * group, group)
        turned = jnp.swapaxes(m_ref[:, pl.ds(first, group), :], 0, 1)
        for i in range(group):
            msend[first + i] = packed(turned[i])

    load.wait()
    each(nz // group, cast)
    xin[0, 0] = msend[z]

    pl.semaphore_wait(barrier, (nz - 1) + (ny - 1) + (nx - 1) + 1)

    def z_copy(d):
        return remote(
            msend.at[lax.rem(z + d, nz)], xin.at[0, d], zs.at[d], zr.at[d], to_z(d)
        )

    def swap_copy(d):
        return remote(xin.at[0, d], xin.at[1, d], cs.at[d], cr.at[d], to_core)

    each(nz - 1, lambda k: z_copy(mixed(k, nz)).start())
    sq_core = remote(sq.at[0], sq.at[1], ss.at[0], sr.at[0], to_core)
    sq_core.start()
    swap_copy(0).start()

    def unpack(side, d):
        rows = pl.ds(pl.multiple_of(side * half + d * 8, 8), 8)
        flat = xin[side, d].astype(f32)
        xe[rows, :short] = jnp.where(row_of(flat.shape) < ROWS, flat, 0.0)
        xe[rows, short:width] = last_block(flat)

    def z_take(k):
        d = mixed_late(k, nz)
        z_copy(d).wait_recv()
        swap_copy(d).start()
        unpack(0, d)

    unpack(0, 0)
    each(nz - 1, z_take)

    def swap_take(d):
        swap_copy(d).wait_recv()
        unpack(1, d)

    swap_take(0)
    each(nz - 1, lambda k: swap_take(mixed_late(k, nz)))
    sq_core.wait_recv()
    sq[2] = sq[0] + sq[1]

    def z_sent(d):
        z_copy(d + 1).wait_send()
        swap_copy(d + 1).wait_send()

    pending.append(lambda: each(nz - 1, z_sent))
    pending.append(swap_copy(0).wait_send)
    pending.append(sq_core.wait_send)

    def sq_x(d):
        return remote(sq.at[2], sq.at[2 + d], ss.at[d], sr.at[d], to_x(d))

    for d in order_x:
        sq_x(d).start()
        pending.append(sq_x(d).wait_send)

    xb[...] = xe[...].astype(bf16)

    def x_copy(j, d):
        return remote(psend.at[j, d], precv.at[j, d], xs.at[j, d], xr.at[j, d], to_x(d))

    def columns(first):
        t = lax.rem(first, nb)
        return xb[:, pl.ds(pl.multiple_of(t * LANES, LANES), LANES)]

    def partial_gram(d):
        first = 2 * lax.rem(x + d, nx) + c
        right = jnp.concatenate([columns(first + j) for j in range(nd)], 1)
        return lax.dot_general(
            columns(first), right, (((0,), (0,)), ((), ())), preferred_element_type=f32
        )

    for d in order_x:
        value = partial_gram(d).astype(bf16)
        for j in range(nd):
            psend[j, d] = value[:, j * LANES : (j + 1) * LANES]
    for j in CHUNKS[:nd]:
        for d in order_x:
            x_copy(j, d).start()
            pending.append(x_copy(j, d).wait_send)
    value = partial_gram(0)
    for j in range(nd):
        own[j] = value[:, j * LANES : (j + 1) * LANES]

    mine = 2 * x + c
    sq_y = remote(sq.at[nx + 2], sq.at[nx + 3], ss.at[nx], sr.at[nx], to_y(ny // 2))
    inverse = []

    def y_copy(j, d):
        return remote(
            qsend.at[j, lax.rem(y + d, ny)], qrecv.at[j, d], ys.at[j, d], yr.at[j, d], to_y(d)
        )

    def gy_copy(j, d, slot):
        return remote(
            stored.at[j, mine, slot], stored.at[j, mine, slot], gys.at[j, d], gyr.at[j, d], to_y(d)
        )

    def gx_copy(j, d, slot):
        return remote(
            stored.at[j, slot], stored.at[j, slot], gxs.at[j, d], gxr.at[j, d], to_x(d)
        )

    def gc_copy(j, d, slot):
        return remote(
            stored.at[j, slot], stored.at[j, slot], gcs.at[j, d], gcr.at[j, d], to_core
        )

    def block_of(d, core):
        return 2 * lax.rem(x + nx - d, nx) + core

    def assemble(j, i):
        rows = pl.ds(pl.multiple_of(i * LANES, LANES), LANES)
        cols = pl.ds(pl.multiple_of(lax.rem(i + j, nb) * LANES, LANES), LANES)
        piece = stored[j, i].reshape(LANES, LANES)
        gram[rows, cols] = piece
        if 0 < j < nd - 1:
            gram[cols, rows] = piece.T

    def step_x(j, first):
        total = own[j]
        for d in reversed(order_x):
            x_copy(j, d).wait_recv()
            total = total + precv[j, d].astype(f32)
        total = total.reshape(acc.shape[1:])
        acc[j] = total
        qsend[j] = total.astype(bf16)
        if first:
            s_sum = sq[2]
            for d in order_x:
                sq_x(d).wait_recv()
                s_sum = s_sum + sq[2 + d]
            sq[nx + 2] = s_sum
            sq_y.start()
            pending.append(sq_y.wait_send)
        each(ny - 1, lambda k: y_copy(j, mixed(k, ny)).start())
        pending.append(lambda: each(ny - 1, lambda k: y_copy(j, k + 1).wait_send()))

    def step_y(j, first):
        if first:
            sq_y.wait_recv()
            square = sq[nx + 2] + sq[nx + 3]
            sq[nx + 4] = square
            inverse.append(jnp.concatenate([1.0 / square] * (part // 8), 0))

        def add(k, total):
            d = mixed_late(k, ny)
            y_copy(j, d).wait_recv()
            return total + qrecv[j, d].astype(f32)

        total = lax.fori_loop(0, ny - 1, add, acc[j, y])
        stored[j, mine, y] = (total * inverse[0]).astype(bf16)
        each(ny - 1, lambda k: gy_copy(j, mixed(k, ny), y).start())
        pending.append(lambda: each(ny - 1, lambda k: gy_copy(j, k + 1, y).wait_send()))

    def step_a(j, first):
        def take(k):
            d = mixed_late(k, ny)
            gy_copy(j, d, lax.rem(y + ny - d, ny)).wait_recv()

        each(ny - 1, take)
        for d in order_x:
            gx_copy(j, d, mine).start()
            pending.append(gx_copy(j, d, mine).wait_send)
        gc_copy(j, 0, mine).start()
        pending.append(gc_copy(j, 0, mine).wait_send)
        assemble(j, mine)

    late = []

    def step_b(j, first):
        for d in reversed(order_x):
            gx_copy(j, d, block_of(d, c)).wait_recv()
            gc_copy(j, d, block_of(d, c)).start()
            pending.append(gc_copy(j, d, block_of(d, c)).wait_send)
            assemble(j, block_of(d, c))
        for k in late:
            others(k)
        late[:] = [j]

    def others(j):
        for d in (0, *reversed(order_x)):
            gc_copy(j, d, block_of(d, 1 - c)).wait_recv()
            assemble(j, block_of(d, 1 - c))

    steps = {"X": step_x, "Y": step_y, "A": step_a, "B": step_b}
    seen = set()
    chunks = [j for j in CHUNKS if j < nd]
    for name in STEPS:
        if int(name[1]) < nd:
            steps[name[0]](chunks[int(name[1])], name[0] not in seen)
            seen.add(name[0])
    for k in late:
        others(k)

    def update_columns(*cuts):
        def joined(ref, rows=slice(None)):
            return jnp.concatenate([ref[rows, cut] for cut in cuts], 1)

        right = joined(gram)
        square_cols = jnp.dot(gram[...], right, preferred_element_type=f32)
        poly[:, : right.shape[1]] = (
            coef_b * right.astype(f32) + coef_c * square_cols
        ).astype(bf16)
        value = coef_a * joined(xe, slice(half)) + jnp.dot(
            xb[:half, :], poly[:, : right.shape[1]], preferred_element_type=f32
        )
        at = 0
        for cut in cuts:
            size = cut.stop - cut.start
            zrow[:, cut] = value[:, at : at + size]
            at += size

    root = jnp.sqrt(f32(C)) / jnp.sqrt(sq[nx + 4])

    def tail_rows(d):
        rows = pl.ds(pl.multiple_of(d * 8, 8), 8)
        tail[rows, :] = spread_rows(zrow[rows, short:] * root)

    def o_copy(q, d, source):
        cols = pl.ds(OUT_CUTS[q], OUT_CUTS[q + 1] - OUT_CUTS[q])
        return remote(
            osend.at[d, :, cols], orecv.at[source, :, cols], os.at[q, d], orv.at[q, d],
            {"z": lax.rem(z + nz - d, nz)},
        )

    def send_back(q, d):
        cols = slice(OUT_CUTS[q], OUT_CUTS[q + 1])
        rows = pl.ds(pl.multiple_of(d * 8, 8), 8)
        scale = jnp.concatenate([root] * ((cols.stop - cols.start) // LANES), 1)
        value = zrow[rows, cols] * scale
        value = jnp.where(row_of(value.shape) < ROWS, value, tail[rows, cols])
        osend[d, :, cols] = value.astype(bf16)

    for q in range(len(OUT_CUTS) - 1):
        cut = slice(OUT_CUTS[q], OUT_CUTS[q + 1])
        if q == 0:
            update_columns(slice(short, width), cut)
            each(nz, tail_rows)
        else:
            update_columns(cut)

        def o_start(k, q=q):
            d = mixed(k, nz)
            send_back(q, d)
            o_copy(q, d, z).start()

        each(nz - 1, o_start)
        send_back(q, 0)

    for wait in pending:
        wait()

    def put(e, value):
        o_ref[e, :, :short] = value
        o_ref[e, :, short:] = last_block(value.astype(f32)).astype(bf16)

    put(z, osend[0])

    def o_take(k):
        d = mixed_late(k, nz)
        source = lax.rem(z + d, nz)
        for q in range(len(OUT_CUTS) - 1):
            o_copy(q, d, source).wait()
        put(source, orecv[source])

    each(nz - 1, o_take)


def on_device(sizes, momentum, spectral_sq):
    nx, ny, nz, _ = sizes
    nb = 2 * nx
    nd = nb // 2 + 1
    rows, width = momentum.shape[1:]
    assert momentum.shape[0] == nz and width == nb * LANES and rows == ROWS
    part = LANES // ny
    short = ROWS * LANES
    nq = len(OUT_CUTS) - 1
    sem = pltpu.SemaphoreType.DMA
    vmem = pltpu.VMEM
    out = pl.pallas_call(
        lambda *refs: kernel(sizes, *refs),
        out_shape=jax.ShapeDtypeStruct((nz, 8, width), bf16),
        in_specs=[
            pl.BlockSpec(memory_space=pltpu.HBM),
            pl.BlockSpec(memory_space=pltpu.SMEM),
        ],
        out_specs=pl.BlockSpec(memory_space=pltpu.VMEM),
        scratch_shapes=[
            vmem((rows, nz, width), f32),
            vmem((nz, 8, short), bf16),
            vmem((2, nz, 8, short), bf16),
            vmem((2 * nz * 8, width), f32),
            vmem((2 * nz * 8, width), bf16),
            vmem((nd, nx, LANES, LANES), bf16),
            vmem((nd, nx, LANES, LANES), bf16),
            vmem((nd, LANES, LANES), f32),
            vmem((nd, ny, part, LANES), f32),
            vmem((nd, ny, part, LANES), bf16),
            vmem((nd, ny, part, LANES), bf16),
            vmem((nd, nb, ny, part, LANES), bf16),
            vmem((width, width), bf16),
            vmem((width, width), bf16),
            vmem((nz * 8, width), f32),
            vmem((nz * 8, short), f32),
            vmem((nz, 8, short), bf16),
            vmem((nz, 8, short), bf16),
            vmem((nx + 5, 8, LANES), f32),
            sem(()),
            sem((nz,)), sem((nz,)), sem((nz,)), sem((nz,)),
            sem((nd, nx)), sem((nd, nx)), sem((nd, ny)), sem((nd, ny)),
            sem((nd, ny)), sem((nd, ny)), sem((nd, nx)), sem((nd, nx)),
            sem((nd, nx)), sem((nd, nx)), sem((nq, nz)), sem((nq, nz)),
            sem((nx + 1,)), sem((nx + 1,)),
        ],
        compiler_params=pltpu.CompilerParams(
            collective_id=0, has_side_effects=True, vmem_limit_bytes=48 << 20
        ),
        name="muon_step",
    )(pltpu.with_memory_space_constraint(momentum.transpose(1, 0, 2), pltpu.HBM), spectral_sq)
    return out[:, :rows]


def solution(mesh):
    ne, nf = mesh.shape["expert"], mesh.shape["fsdp"]
    nx, nyl = ne // 4, 4
    nz = nf // nyl
    sizes = (nx, 2 * nyl, nz, nyl)
    finer = Mesh(mesh.devices.reshape(nx, 2, 2, nyl, nz), AXES)
    rows = P(None, ("yl", "z", "x", "yh", "core"), None)
    return jax.shard_map(
        lambda m, s: on_device(sizes, m, s),
        mesh=finer,
        in_specs=(rows, P(("x", "yh", "core"))),
        out_specs=rows,
        check_vma=False,
    )
```

```python
import jax
import jax.numpy as jnp
from jax import lax
from jax.experimental import pallas as pl
from jax.experimental.pallas import tpu as pltpu
from jax.sharding import Mesh
from jax.sharding import PartitionSpec as P

C = 7168
coef_a = 3.4445
coef_b = -4.775
coef_c = 2.0315

AXES = ("x", "yh", "core", "yl", "z")
MESH = pl.DeviceIdType.MESH
LANES = 128
ROWS = 7
f32 = jnp.float32
bf16 = jnp.bfloat16

CHUNKS = (1, 2, 3, 4, 0)
STEPS = (
    "X0", "X1", "X2", "Y0", "X3", "Y1", "X4", "Y2", "A0", "Y3",
    "A1", "Y4", "A2", "B0", "A3", "B1", "A4", "B2", "B3", "B4",
)
OUT_CUTS = (0, 384, 896)


def row_of(shape):
    return lax.broadcasted_iota(jnp.int32, shape, 0)


def spread_rows(last):
    return jnp.concatenate(
        [jnp.broadcast_to(last[j : j + 1], (8, LANES)) for j in range(ROWS)], 1
    )


def last_block(packed):
    out = jnp.zeros((8, LANES), f32)
    row = row_of(out.shape)
    for j in range(ROWS):
        piece = packed[ROWS : ROWS + 1, j * LANES : (j + 1) * LANES]
        out = jnp.where(row == j, jnp.broadcast_to(piece, out.shape), out)
    return out


def kernel(
    sizes, m_hbm, s_ref, o_ref,
    m_ref, msend, xin, xe, xb, psend, precv, own, acc, qsend, qrecv,
    stored, gram, poly, zrow, tail, osend, orecv, sq,
    m_sem, zs, zr, cs, cr, xs, xr, ys, yr, gys, gyr, gxs, gxr, gcs, gcr, os, orv,
    ss, sr,
):
    nx, ny, nz, nyl = sizes
    nb = 2 * nx
    nd = nb // 2 + 1
    x, yh, c, yl, z = [lax.axis_index(a) for a in AXES]
    y = yh * nyl + yl
    expert = (x * 2 + yh) * 2 + c
    part = LANES // ny
    width = nb * LANES
    short = ROWS * LANES
    half = nz * 8
    order_x = sorted(range(1, nx), key=lambda d: -min(d, nx - d))
    pending = []

    def to_z(d):
        return {"z": lax.rem(z + d, nz)}

    def to_x(d):
        return {"x": lax.rem(x + d, nx)}

    def to_y(d):
        t = lax.rem(y + d, ny)
        return {"yh": t // nyl, "yl": lax.rem(t, nyl)}

    to_core = {"core": 1 - c}

    def mixed(k, n):
        g, r = jnp.maximum(k - 1, 0) // 4, lax.rem(jnp.maximum(k - 1, 0), 4)
        near = 1 + g + lax.rem(r, 2) * (n - 2 - 2 * g)
        far = n // 2 - 1 - g + lax.rem(r, 2) * (2 + 2 * g)
        return jnp.where(k == 0, n // 2, jnp.where(r < 2, near, far))

    def mixed_late(k, n):
        return mixed(lax.rem(k + 1, n - 1), n)

    def each(n, body):
        def step(k, carry):
            body(k)
            return carry

        lax.fori_loop(0, n, step, 0)

    def remote(src, dst, send_sem, recv_sem, where):
        return pltpu.make_async_remote_copy(
            src_ref=src, dst_ref=dst, send_sem=send_sem, recv_sem=recv_sem,
            device_id=where, device_id_type=MESH,
        )

    load = pltpu.make_async_copy(m_hbm, m_ref, m_sem)
    load.start()

    barrier = pltpu.get_barrier_semaphore()

    def greet(where):
        pl.semaphore_signal(barrier, inc=1, device_id=where, device_id_type=MESH)

    each(nz - 1, lambda k: greet(to_z(mixed(k, nz))))
    each(ny - 1, lambda k: greet(to_y(mixed(k, ny))))
    for d in order_x:
        greet(to_x(d))
    greet(to_core)

    sq[0] = jnp.full(sq.shape[1:], jnp.where(expert == z, s_ref[0], 0.0), f32)

    def packed(rows):
        end = jnp.concatenate([rows[j : j + 1, short:] for j in range(ROWS)], 1)
        return jnp.concatenate([rows[:, :short], end], 0).astype(bf16)

    group = min(nz, 8)

    def cast(g):
        first = pl.multiple_of(g * group, group)
        turned = jnp.swapaxes(m_ref[:, pl.ds(first, group), :], 0, 1)
        for i in range(group):
            msend[first + i] = packed(turned[i])

    load.wait()
    each(nz // group, cast)
    xin[0, 0] = msend[z]

    pl.semaphore_wait(barrier, (nz - 1) + (ny - 1) + (nx - 1) + 1)

    def z_copy(d):
        return remote(
            msend.at[lax.rem(z + d, nz)], xin.at[0, d], zs.at[d], zr.at[d], to_z(d)
        )

    def swap_copy(d):
        return remote(xin.at[0, d], xin.at[1, d], cs.at[d], cr.at[d], to_core)

    each(nz - 1, lambda k: z_copy(mixed(k, nz)).start())
    sq_core = remote(sq.at[0], sq.at[1], ss.at[0], sr.at[0], to_core)
    sq_core.start()
    swap_copy(0).start()

    def unpack(side, d):
        rows = pl.ds(pl.multiple_of(side * half + d * 8, 8), 8)
        flat = xin[side, d].astype(f32)
        xe[rows, :short] = jnp.where(row_of(flat.shape) < ROWS, flat, 0.0)
        xe[rows, short:width] = last_block(flat)

    def z_take(k):
        d = mixed_late(k, nz)
        z_copy(d).wait_recv()
        swap_copy(d).start()
        unpack(0, d)

    unpack(0, 0)

    def swap_take(d):
        swap_copy(d).wait_recv()
        unpack(1, d)

    lag = min(4, nz - 1)
    each(lag, z_take)
    swap_take(0)

    def both(k):
        z_take(k + lag)
        swap_take(mixed_late(k, nz))

    each(nz - 1 - lag, both)
    each(lag, lambda k: swap_take(mixed_late(k + nz - 1 - lag, nz)))
    sq_core.wait_recv()
    sq[2] = sq[0] + sq[1]

    def z_sent(d):
        z_copy(d + 1).wait_send()
        swap_copy(d + 1).wait_send()

    pending.append(lambda: each(nz - 1, z_sent))
    pending.append(swap_copy(0).wait_send)
    pending.append(sq_core.wait_send)

    def sq_x(d):
        return remote(sq.at[2], sq.at[2 + d], ss.at[d], sr.at[d], to_x(d))

    for d in order_x:
        sq_x(d).start()
        pending.append(sq_x(d).wait_send)

    xb[...] = xe[...].astype(bf16)

    def x_copy(j, d):
        return remote(psend.at[j, d], precv.at[j, d], xs.at[j, d], xr.at[j, d], to_x(d))

    def columns(first):
        t = lax.rem(first, nb)
        return xb[:, pl.ds(pl.multiple_of(t * LANES, LANES), LANES)]

    def partial_gram(d):
        first = 2 * lax.rem(x + d, nx) + c
        right = jnp.concatenate([columns(first + j) for j in range(nd)], 1)
        return lax.dot_general(
            columns(first), right, (((0,), (0,)), ((), ())), preferred_element_type=f32
        )

    for d in order_x:
        value = partial_gram(d).astype(bf16)
        for j in range(nd):
            psend[j, d] = value[:, j * LANES : (j + 1) * LANES]
    for j in CHUNKS[:nd]:
        for d in order_x:
            x_copy(j, d).start()
            pending.append(x_copy(j, d).wait_send)
    value = partial_gram(0)
    for j in range(nd):
        own[j] = value[:, j * LANES : (j + 1) * LANES]

    mine = 2 * x + c
    sq_y = remote(sq.at[nx + 2], sq.at[nx + 3], ss.at[nx], sr.at[nx], to_y(ny // 2))
    inverse = []

    def y_copy(j, d):
        return remote(
            qsend.at[j, lax.rem(y + d, ny)], qrecv.at[j, d], ys.at[j, d], yr.at[j, d], to_y(d)
        )

    def gy_copy(j, d, slot):
        return remote(
            stored.at[j, mine, slot], stored.at[j, mine, slot], gys.at[j, d], gyr.at[j, d], to_y(d)
        )

    def gx_copy(j, d, slot):
        return remote(
            stored.at[j, slot], stored.at[j, slot], gxs.at[j, d], gxr.at[j, d], to_x(d)
        )

    def gc_copy(j, d, slot):
        return remote(
            stored.at[j, slot], stored.at[j, slot], gcs.at[j, d], gcr.at[j, d], to_core
        )

    def block_of(d, core):
        return 2 * lax.rem(x + nx - d, nx) + core

    def assemble(j, i):
        rows = pl.ds(pl.multiple_of(i * LANES, LANES), LANES)
        cols = pl.ds(pl.multiple_of(lax.rem(i + j, nb) * LANES, LANES), LANES)
        piece = stored[j, i].reshape(LANES, LANES)
        gram[rows, cols] = piece
        if 0 < j < nd - 1:
            gram[cols, rows] = piece.T

    def step_x(j, first):
        total = own[j]
        for d in reversed(order_x):
            x_copy(j, d).wait_recv()
            total = total + precv[j, d].astype(f32)
        total = total.reshape(acc.shape[1:])
        acc[j] = total
        qsend[j] = total.astype(bf16)
        if first:
            s_sum = sq[2]
            for d in order_x:
                sq_x(d).wait_recv()
                s_sum = s_sum + sq[2 + d]
            sq[nx + 2] = s_sum
            sq_y.start()
            pending.append(sq_y.wait_send)
        each(ny - 1, lambda k: y_copy(j, mixed(k, ny)).start())
        pending.append(lambda: each(ny - 1, lambda k: y_copy(j, k + 1).wait_send()))

    def step_y(j, first):
        if first:
            sq_y.wait_recv()
            square = sq[nx + 2] + sq[nx + 3]
            sq[nx + 4] = square
            inverse.append(jnp.concatenate([1.0 / square] * (part // 8), 0))

        def add(k, total):
            d = mixed_late(k, ny)
            y_copy(j, d).wait_recv()
            return total + qrecv[j, d].astype(f32)

        total = lax.fori_loop(0, ny - 1, add, acc[j, y])
        stored[j, mine, y] = (total * inverse[0]).astype(bf16)
        each(ny - 1, lambda k: gy_copy(j, mixed(k, ny), y).start())
        pending.append(lambda: each(ny - 1, lambda k: gy_copy(j, k + 1, y).wait_send()))

    def step_a(j, first):
        def take(k):
            d = mixed_late(k, ny)
            gy_copy(j, d, lax.rem(y + ny - d, ny)).wait_recv()

        each(ny - 1, take)
        for d in order_x:
            gx_copy(j, d, mine).start()
            pending.append(gx_copy(j, d, mine).wait_send)
        gc_copy(j, 0, mine).start()
        pending.append(gc_copy(j, 0, mine).wait_send)
        assemble(j, mine)

    late = []

    def step_b(j, first):
        for d in reversed(order_x):
            gx_copy(j, d, block_of(d, c)).wait_recv()
            gc_copy(j, d, block_of(d, c)).start()
            pending.append(gc_copy(j, d, block_of(d, c)).wait_send)
            assemble(j, block_of(d, c))
        for k in late:
            others(k)
        late[:] = [j]

    def others(j):
        for d in (0, *reversed(order_x)):
            gc_copy(j, d, block_of(d, 1 - c)).wait_recv()
            assemble(j, block_of(d, 1 - c))

    steps = {"X": step_x, "Y": step_y, "A": step_a, "B": step_b}
    seen = set()
    chunks = [j for j in CHUNKS if j < nd]
    for name in STEPS:
        if int(name[1]) < nd:
            steps[name[0]](chunks[int(name[1])], name[0] not in seen)
            seen.add(name[0])
    for k in late:
        others(k)

    def update_columns(*cuts):
        def joined(ref, rows=slice(None)):
            return jnp.concatenate([ref[rows, cut] for cut in cuts], 1)

        right = joined(gram)
        square_cols = jnp.dot(gram[...], right, preferred_element_type=f32)
        poly[:, : right.shape[1]] = (
            coef_b * right.astype(f32) + coef_c * square_cols
        ).astype(bf16)
        value = coef_a * joined(xe, slice(half)) + jnp.dot(
            xb[:half, :], poly[:, : right.shape[1]], preferred_element_type=f32
        )
        at = 0
        for cut in cuts:
            size = cut.stop - cut.start
            zrow[:, cut] = value[:, at : at + size]
            at += size

    root = jnp.sqrt(f32(C)) / jnp.sqrt(sq[nx + 4])

    def tail_rows(d):
        rows = pl.ds(d * 8, 8)
        tail[rows, :] = spread_rows(zrow[rows, short:] * root)

    def o_copy(q, d, source):
        cols = pl.ds(OUT_CUTS[q], OUT_CUTS[q + 1] - OUT_CUTS[q])
        return remote(
            osend.at[d, :, cols], orecv.at[source, :, cols], os.at[q, d], orv.at[q, d],
            {"z": lax.rem(z + nz - d, nz)},
        )

    def send_back(q, d):
        cols = slice(OUT_CUTS[q], OUT_CUTS[q + 1])
        rows = pl.ds(pl.multiple_of(d * 8, 8), 8)
        scale = jnp.concatenate([root] * ((cols.stop - cols.start) // LANES), 1)
        value = zrow[rows, cols] * scale
        value = jnp.where(row_of(value.shape) < ROWS, value, tail[rows, cols])
        osend[d, :, cols] = value.astype(bf16)

    for q in range(len(OUT_CUTS) - 1):
        cut = slice(OUT_CUTS[q], OUT_CUTS[q + 1])
        if q == 0:
            update_columns(slice(short, width), cut)
            for d in range(nz):
                tail_rows(d)
        else:
            update_columns(cut)

        def o_start(k, q=q):
            d = mixed(k, nz)
            send_back(q, d)
            o_copy(q, d, z).start()

        each(nz - 1, o_start)
        send_back(q, 0)

    for wait in pending:
        wait()

    def put(e, value):
        o_ref[e, :, :short] = value
        o_ref[e, :, short:] = last_block(value.astype(f32)).astype(bf16)

    put(z, osend[0])

    def o_take(k):
        d = mixed_late(k, nz)
        source = lax.rem(z + d, nz)
        for q in range(len(OUT_CUTS) - 1):
            o_copy(q, d, source).wait()
        put(source, orecv[source])

    each(nz - 1, o_take)


def on_device(sizes, momentum, spectral_sq):
    nx, ny, nz, _ = sizes
    nb = 2 * nx
    nd = nb // 2 + 1
    rows, width = momentum.shape[1:]
    assert momentum.shape[0] == nz and width == nb * LANES and rows == ROWS
    part = LANES // ny
    short = ROWS * LANES
    nq = len(OUT_CUTS) - 1
    sem = pltpu.SemaphoreType.DMA
    vmem = pltpu.VMEM
    out = pl.pallas_call(
        lambda *refs: kernel(sizes, *refs),
        out_shape=jax.ShapeDtypeStruct((nz, 8, width), bf16),
        in_specs=[
            pl.BlockSpec(memory_space=pltpu.HBM),
            pl.BlockSpec(memory_space=pltpu.SMEM),
        ],
        out_specs=pl.BlockSpec(memory_space=pltpu.VMEM),
        scratch_shapes=[
            vmem((rows, nz, width), f32),
            vmem((nz, 8, short), bf16),
            vmem((2, nz, 8, short), bf16),
            vmem((2 * nz * 8, width), f32),
            vmem((2 * nz * 8, width), bf16),
            vmem((nd, nx, LANES, LANES), bf16),
            vmem((nd, nx, LANES, LANES), bf16),
            vmem((nd, LANES, LANES), f32),
            vmem((nd, ny, part, LANES), f32),
            vmem((nd, ny, part, LANES), bf16),
            vmem((nd, ny, part, LANES), bf16),
            vmem((nd, nb, ny, part, LANES), bf16),
            vmem((width, width), bf16),
            vmem((width, width), bf16),
            vmem((nz * 8, width), f32),
            vmem((nz * 8, short), f32),
            vmem((nz, 8, short), bf16),
            vmem((nz, 8, short), bf16),
            vmem((nx + 5, 8, LANES), f32),
            sem(()),
            sem((nz,)), sem((nz,)), sem((nz,)), sem((nz,)),
            sem((nd, nx)), sem((nd, nx)), sem((nd, ny)), sem((nd, ny)),
            sem((nd, ny)), sem((nd, ny)), sem((nd, nx)), sem((nd, nx)),
            sem((nd, nx)), sem((nd, nx)), sem((nq, nz)), sem((nq, nz)),
            sem((nx + 1,)), sem((nx + 1,)),
        ],
        compiler_params=pltpu.CompilerParams(
            collective_id=0, has_side_effects=True, vmem_limit_bytes=48 << 20
        ),
        name="muon_step",
    )(pltpu.with_memory_space_constraint(momentum.transpose(1, 0, 2), pltpu.HBM), spectral_sq)
    return out[:, :rows]


def solution(mesh):
    ne, nf = mesh.shape["expert"], mesh.shape["fsdp"]
    nx, nyl = ne // 4, 4
    nz = nf // nyl
    sizes = (nx, 2 * nyl, nz, nyl)
    finer = Mesh(mesh.devices.reshape(nx, 2, 2, nyl, nz), AXES)
    rows = P(None, ("yl", "z", "x", "yh", "core"), None)
    return jax.shard_map(
        lambda m, s: on_device(sizes, m, s),
        mesh=finer,
        in_specs=(rows, P(("x", "yh", "core"))),
        out_specs=rows,
        check_vma=False,
    )
```
